16 devices in a mesh: dp: 2 (over y, z), tp: 8 (over x, core).
Axes of the slice: x: 4, y: 2, z: 1, core: 2. Of those that a mesh axis runs over, the one named last changes fastest.
The devices are a block of a 4x4x8 slice.
Arguments:
- x: bfloat16 [8, 512, 8192], P('dp'), parts along dimension 0
- gain_a: bfloat16 [8192], replicated
- wq: bfloat16 [8192, 8192], P(None, 'tp')
- wk: bfloat16 [8192, 1024], P(None, 'tp')
- wv: bfloat16 [8192, 1024], P(None, 'tp')
- wo: bfloat16 [8192, 8192], P('tp')
- gain_m: bfloat16 [8192], replicated
- w_gate: bfloat16 [8192, 28672], P(None, 'tp')
- w_up: bfloat16 [8192, 28672], P(None, 'tp')
- w_down: bfloat16 [28672, 8192], P('tp')
Outputs:
- output: bfloat16 [8, 512, 8192], P('dp'), parts along dimension 0
There are 2 independent parts. The reference program is written for one: setup_inputs(seed, part) draws one part's arguments, and reference() takes and returns one part's arrays. A program takes and returns all parts, laid end to end along the dimension named above; an argument that names none is the same for every part.
All inputs are finite; a program needn't handle non-finite values.
Results may differ from the reference program's by a relative error of at most 0.017.
Values are sent between devices in bfloat16 or wider.
A program may use at most 768 MiB of HBM per device.

```python
import jax
import jax.numpy as jnp
from jax import lax

SEQUENCES = 4
TOKENS = 512
D = 8192
HEADS = 64
KV_HEADS = 8
HEAD = 128
FF = 28672
THETA = 10000


def setup_inputs(seed: int = 0, part: int = 0) -> dict:
    kx, ka, km, kq, kk, kv, ko, kg, ku, kd = jax.random.split(jax.random.key(seed), 10)

    def weights(key, rows, columns):
        return jax.random.normal(key, (rows, columns), jnp.float32) * rows**-0.5

    drawn = {
        "x": jax.random.normal(jax.random.fold_in(kx, part), (SEQUENCES, TOKENS, D), jnp.float32),
        "gain_a": 1 + 0.1 * jax.random.normal(ka, (D,), jnp.float32),
        "wq": 2 * weights(kq, D, HEADS * HEAD),
        "wk": 2 * weights(kk, D, KV_HEADS * HEAD),
        "wv": 4 * weights(kv, D, KV_HEADS * HEAD),
        "wo": weights(ko, HEADS * HEAD, D),
        "gain_m": 1 + 0.1 * jax.random.normal(km, (D,), jnp.float32),
        "w_gate": weights(kg, D, FF),
        "w_up": weights(ku, D, FF),
        "w_down": 3 * weights(kd, FF, D),
    }
    return {k: v.astype(jnp.bfloat16) for k, v in drawn.items()}


def normed(x, gain):
    wide = x.astype(jnp.float32)
    scale = lax.rsqrt(jnp.mean(wide * wide, -1, keepdims=True) + 1e-6)
    return (wide * scale * gain.astype(jnp.float32)).astype(jnp.bfloat16)


def turned(t, place, theta):
    half = t.shape[-1] // 2
    angle = place.astype(jnp.float32)[:, None] * theta ** (-jnp.arange(half, dtype=jnp.float32) / half)
    cos, sin = jnp.cos(angle)[:, None], jnp.sin(angle)[:, None]
    a, b = t[..., :half].astype(jnp.float32), t[..., half:].astype(jnp.float32)
    return jnp.concatenate([a * cos - b * sin, b * cos + a * sin], -1).astype(jnp.bfloat16)


def matmul(a, w):
    return jnp.dot(a, w, preferred_element_type=jnp.float32).astype(jnp.bfloat16)


def einsum(form, a, b):
    return jnp.einsum(form, a.astype(jnp.float32), b.astype(jnp.float32))


def attention(q, k, v):
    scores = einsum("tgsd,ugd->gstu", q, k) * q.shape[-1] ** -0.5
    token = jnp.arange(q.shape[0])
    scores = jnp.where(token[:, None] >= token, scores, -jnp.inf)
    weights = jax.nn.softmax(scores, -1).astype(jnp.bfloat16)
    return einsum("gstu,ugd->tgsd", weights, v).astype(jnp.bfloat16)


def one(x, gain_a, wq, wk, wv, wo, gain_m, w_gate, w_up, w_down):
    rows = x.shape[0]
    a, place = normed(x, gain_a), jnp.arange(rows)
    k = turned(matmul(a, wk).reshape(rows, -1, HEAD), place, THETA)
    q = turned(matmul(a, wq).reshape(rows, -1, HEAD), place, THETA).reshape(rows, k.shape[1], -1, HEAD)
    v = matmul(a, wv).reshape(rows, -1, HEAD)
    seen = attention(q, k, v).reshape(rows, -1)
    h = (x.astype(jnp.float32) + jnp.dot(seen, wo, preferred_element_type=jnp.float32)).astype(jnp.bfloat16)
    b = normed(h, gain_m)
    gate = jnp.dot(b, w_gate, preferred_element_type=jnp.float32)
    up = jnp.dot(b, w_up, preferred_element_type=jnp.float32)
    hidden = (jax.nn.silu(gate) * up).astype(jnp.bfloat16)
    return (h.astype(jnp.float32) + jnp.dot(hidden, w_down, preferred_element_type=jnp.float32)).astype(jnp.bfloat16)


def reference(x, gain_a, wq, wk, wv, wo, gain_m, w_gate, w_up, w_down):
    return lax.map(lambda sequence: one(sequence, gain_a, wq, wk, wv, wo, gain_m, w_gate, w_up, w_down), x)
```

```python
import functools

import jax
import jax.numpy as jnp
from jax import lax
from jax.experimental import pallas as pl
from jax.experimental.pallas import tpu as pltpu
from jax.sharding import PartitionSpec as P

HEAD = 128
THETA = 10000
WIDE = 2 * HEAD
DEPTH = 2048
STRIP = 16
SPAN = 1024
OUT = 1024
QUERIES = 128


def _dot(a, b, ca=1, cb=0):
    return lax.dot_general(a, b, (((ca,), (cb,)), ((), ())), preferred_element_type=jnp.float32)


def _attention_kernel(steps, x_ref, gain_ref, turn_ref, wk_ref, wv_ref, wq_ref, wo_ref, o_ref, a_s, k_s, v_s, acc_s, seen_s):
    rows, d = a_s.shape

    def project(w):
        def part(i, _):
            at = pl.ds(pl.multiple_of(i * DEPTH, DEPTH), DEPTH)
            acc_s[...] += _dot(a_s[:, at], w(at))
            return _

        acc_s[...] = jnp.zeros_like(acc_s)
        lax.fori_loop(0, d // DEPTH, part, None)

    def turned(t):
        return (t * turn_ref[0] + pltpu.roll(t, HEAD // 2, 1) * turn_ref[1]).astype(jnp.bfloat16)

    def rounded(at):
        return acc_s[:, at : at + HEAD].astype(jnp.bfloat16)

    @pl.when(pl.program_id(0) == 0)
    def _():
        def strip(i, _):
            here = pl.ds(pl.multiple_of(i * STRIP, STRIP), STRIP)
            squares = jnp.zeros((STRIP, SPAN), jnp.float32)
            for at in range(0, d, SPAN):
                wide = x_ref[0, here, at : at + SPAN].astype(jnp.float32)
                squares += wide * wide
            scale = lax.rsqrt(jnp.sum(squares, -1, keepdims=True) / d + 1e-6)
            for at in range(0, d, SPAN):
                wide = x_ref[0, here, at : at + SPAN].astype(jnp.float32)
                a_s[here, at : at + SPAN] = (wide * scale * gain_ref[:, at : at + SPAN]).astype(jnp.bfloat16)
            return _

        lax.fori_loop(0, rows // STRIP, strip, None)
        project(lambda at: jnp.concatenate([wk_ref[at, :], wv_ref[at, :]], axis=1))
        k_s[...] = turned(rounded(0).astype(jnp.float32))
        v_s[...] = acc_s[:, HEAD : 2 * HEAD].T.astype(jnp.bfloat16)

    step = pl.program_id(0)

    @pl.when((step > 0) & (step <= steps))
    def _():
        project(lambda at: wq_ref[at, :])
        heads = range(0, WIDE, HEAD)
        q = [turned(rounded(head).astype(jnp.float32)) for head in heads]
        for at in range(0, rows, QUERIES):
            end = at + QUERIES
            scores = _dot(k_s[:end, :], jnp.concatenate([t[at:end] for t in q], axis=0), 1, 1) * HEAD**-0.5
            key = lax.broadcasted_iota(jnp.int32, scores.shape, 0)
            query = lax.rem(lax.broadcasted_iota(jnp.int32, scores.shape, 1), QUERIES) + at
            scores = jnp.where(query >= key, scores, -jnp.inf)
            weights = jnp.exp(scores - scores.max(0, keepdims=True))
            weights = (weights * (1 / weights.sum(0, keepdims=True))).astype(jnp.bfloat16)
            out = _dot(v_s[:, :end], weights).T.astype(jnp.bfloat16)
            for n, head in enumerate(heads):
                seen_s[step - 1, at:end, head : head + HEAD] = out[n * QUERIES : (n + 1) * QUERIES]

    @pl.when(step > steps)
    def _():
        seen = jnp.concatenate([seen_s[i] for i in range(seen_s.shape[0])], axis=1)
        for at in range(0, o_ref.shape[1], WIDE):
            o_ref[:, at : at + WIDE] = _dot(seen, wo_ref[:, at : at + WIDE]).astype(o_ref.dtype)


def attended(x, i, gain, turn, wq, wk, wv, wo):
    _, rows, d = x.shape
    steps = wq.shape[1] // WIDE
    blocks = d // OUT
    late = lambda j: jnp.clip(j - 1, 0, steps - 1)
    last = lambda j: jnp.maximum(j - 1 - steps, 0)
    once = pl.Buffered(1)
    whole = lambda a: pl.BlockSpec(a.shape, lambda j: (0,) * a.ndim, pipeline_mode=once)
    return pl.pallas_call(
        functools.partial(_attention_kernel, steps),
        grid=(1 + steps + blocks,),
        in_specs=[
            pl.BlockSpec((1, rows, d), lambda j: (i, 0, 0), pipeline_mode=once),
            *(whole(a) for a in (gain, turn, wk, wv)),
            pl.BlockSpec((d, WIDE), lambda j: (0, late(j))),
            pl.BlockSpec((wo.shape[0], OUT), lambda j: (0, last(j))),
        ],
        out_specs=pl.BlockSpec((rows, OUT), lambda j: (0, last(j))),
        out_shape=jax.ShapeDtypeStruct((rows, d), jnp.bfloat16),
        scratch_shapes=[pltpu.VMEM((rows, d), jnp.bfloat16), pltpu.VMEM((rows, HEAD), jnp.bfloat16), pltpu.VMEM((HEAD, rows), jnp.bfloat16),
                        pltpu.VMEM((rows, WIDE), jnp.float32), pltpu.VMEM((steps, rows, WIDE), jnp.bfloat16)],
        compiler_params=pltpu.CompilerParams(dimension_semantics=("arbitrary",), vmem_limit_bytes=48 * 2**20),
        cost_estimate=pl.CostEstimate(flops=2 * rows * d * (2 * steps + 1) * WIDE, transcendentals=0, bytes_accessed=2 * d * (2 * rows + (2 * steps + 1) * WIDE)),
    )(x, gain, turn, wk, wv, wq, wo)


def _gated_kernel(b_ref, gate_ref, up_ref, o_ref):
    gate, up = _dot(b_ref[...], gate_ref[...]), _dot(b_ref[...], up_ref[...])
    o_ref[...] = (jax.nn.silu(gate) * up).astype(o_ref.dtype)


def gated(b, w_gate, w_up, part=0, parts=1):
    (rows, d), columns = b.shape, w_gate.shape[1] // parts
    blocks = columns // WIDE
    weight = pl.BlockSpec((d, WIDE), lambda j: (0, j + part * blocks))
    return pl.pallas_call(
        _gated_kernel,
        grid=(blocks,),
        in_specs=[pl.BlockSpec((rows, d), lambda j: (0, 0), pipeline_mode=pl.Buffered(1)), weight, weight],
        out_specs=pl.BlockSpec((rows, WIDE), lambda j: (0, j)),
        out_shape=jax.ShapeDtypeStruct((rows, columns), jnp.bfloat16),
        compiler_params=pltpu.CompilerParams(dimension_semantics=("arbitrary",), vmem_limit_bytes=48 * 2**20),
        cost_estimate=pl.CostEstimate(flops=4 * rows * d * columns, transcendentals=rows * columns, bytes_accessed=2 * d * (rows + 2 * columns)),
    )(b, w_gate, w_up)


def _down_kernel(low_ref, high_ref, w_ref, o_ref):
    depth = low_ref.shape[1]
    o_ref[...] = (_dot(low_ref[...], w_ref[:depth, :]) + _dot(high_ref[...], w_ref[depth:, :])).astype(o_ref.dtype)


def downed(low, high, w, part=0, parts=1):
    rows, depth, columns = low.shape[0], w.shape[0] // 2, w.shape[1] // parts
    blocks = columns // OUT
    hidden = lambda at: pl.BlockSpec((rows, depth), lambda j: (0, at), pipeline_mode=pl.Buffered(1))
    return pl.pallas_call(
        _down_kernel,
        grid=(blocks,),
        in_specs=[hidden(0), hidden(int(high is None)), pl.BlockSpec((2 * depth, OUT), lambda j: (0, j + part * blocks))],
        out_specs=pl.BlockSpec((rows, OUT), lambda j: (0, j)),
        out_shape=jax.ShapeDtypeStruct((rows, columns), jnp.bfloat16),
        compiler_params=pltpu.CompilerParams(dimension_semantics=("arbitrary",), vmem_limit_bytes=48 * 2**20),
        cost_estimate=pl.CostEstimate(flops=4 * rows * depth * columns, transcendentals=0, bytes_accessed=4 * depth * (rows + columns)),
    )(low, low if high is None else high, w)


def _place_kernel(part_ref, *rest):
    rest[-1][0] = part_ref[...]


def placed(y, part, batch, i, at, d):
    rows, columns = part.shape
    size = rows // 8
    return pl.pallas_call(
        _place_kernel,
        grid=(rows // size,),
        in_specs=[pl.BlockSpec((size, columns), lambda j: (j, 0)), *([] if y is None else [pl.BlockSpec(memory_space=pl.ANY)])],
        out_specs=pl.BlockSpec((1, size, columns), lambda j: (i, j, at // columns)),
        out_shape=jax.ShapeDtypeStruct((batch, rows, d), part.dtype),
        input_output_aliases={} if y is None else {1: 0},
        compiler_params=pltpu.CompilerParams(dimension_semantics=("arbitrary",)),
        cost_estimate=pl.CostEstimate(flops=8 * rows * d, transcendentals=0, bytes_accessed=4 * rows * columns),
    )(part, *([] if y is None else [y]))


def tables(rows):
    half = HEAD // 2
    angle = jnp.arange(rows).astype(jnp.float32)[:, None] * THETA ** (-jnp.arange(half, dtype=jnp.float32) / half)
    cos, sin = jnp.cos(angle), jnp.sin(angle)
    return jnp.stack([jnp.concatenate([cos, cos], -1), jnp.concatenate([-sin, sin], -1)])


def normed(x, gain):
    wide = x.astype(jnp.float32)
    scale = lax.rsqrt(jnp.mean(wide * wide, -1, keepdims=True) + 1e-6)
    return (wide * scale * gain.astype(jnp.float32)).astype(jnp.bfloat16)


def matmul(a, w):
    return jnp.dot(a, w, preferred_element_type=jnp.float32).astype(jnp.bfloat16)


def wide(t):
    return t.astype(jnp.float32)


def solution(mesh):
    n = mesh.shape["tp"]
    pair = [(i, i ^ 1) for i in range(n)]
    right, left = ([(i, (i + by) % n) for i in range(n)] for by in (2, n - 2))

    def send(t, to):
        return lax.ppermute(t.astype(jnp.bfloat16), "tp", to)

    class Sum:
        def __init__(self, term, after=None):
            me = lax.axis_index("tp")
            self.chip, self.core = me // 2, me % 2
            self.blocks = term.reshape(n // 2, 2, -1, term.shape[-1])
            self.half = self.blocks.shape[2] // 2
            theirs = lax.dynamic_index_in_dim(self.blocks, 1 - self.core, 1, False)
            if after is not None:
                theirs, after = lax.optimization_barrier((theirs, after))
            self.got, self.after = send(theirs, pair), after

        def own(self, got, away, first=True, last=True):
            at = (self.chip + away) % (n // 2)
            low, rows = 0 if first else self.half, self.half * (first + last)
            d = got.shape[-1]
            mine = lax.dynamic_slice(self.blocks, (at, self.core, low, 0), (1, 1, rows, d)).reshape(rows, d)
            return wide(mine) + wide(lax.dynamic_slice(got, (at, low, 0), (1, rows, d)).reshape(rows, d))

        def far(self, got):
            return tuple(self.own(got, 2, *which).astype(jnp.bfloat16) for which in ((True, False), (False, True)))

        def send_far(self, far):
            return send(far[0], right), send(far[1], left)

        def near(self, got, far):
            to_right = jnp.concatenate([self.own(got, 1, last=False) + wide(far[0]), self.own(got, 1, first=False)])
            to_left = jnp.concatenate([self.own(got, -1, last=False), self.own(got, -1, first=False) + wide(far[1])])
            return to_right.astype(jnp.bfloat16), to_left.astype(jnp.bfloat16)

        def send_near(self, near):
            return send(near[0], right), send(near[1], left)

        def total(self, got, near):
            return self.own(got, 0) + wide(near[0]) + wide(near[1])

    class Spread:
        def __init__(self, part):
            self.share = part.shape[0]
            self.mine = part
            self.near = send(part, right), send(part, left)
            self.here = [(0, 0, part)]
            self.there = [(0, 0, send(part, pair))]

        def forward(self):
            half = self.share // 2
            near = lax.optimization_barrier(self.near)
            passed = lax.optimization_barrier((near[0][:half], near[1][half:]))
            far = send(passed[0], right), send(passed[1], left)
            for away, low, rows in ((-1, 0, near[0]), (1, 0, near[1]), (2, 0, far[0]), (2, half, far[1])):
                self.here.append((away, low, rows))
                self.there.append((away, low, send(rows, pair)))

        def pieces(self):
            me = lax.axis_index("tp")
            chip, core = me // 2, me % 2
            for side, pieces in ((core, self.here), (1 - core, self.there)):
                for away, low, rows in pieces:
                    yield (2 * ((chip + away) % (n // 2)) + side) * self.share + low, rows

    def scattered(term):
        return lax.psum_scatter(term, "tp", scatter_dimension=0, tiled=True)

    def gathered(part):
        return lax.all_gather(part, "tp", axis=0, tiled=True)

    def step(x, gain_a, wq, wk, wv, wo, gain_m, w_gate, w_up, w_down):
        batch, rows, d = x.shape
        me, share = lax.axis_index("tp"), rows // n
        turn = tables(rows)
        gain = wide(gain_a)[None]
        tie = lax.optimization_barrier
        hs, bs, sums = [None] * batch, [None] * batch, [None] * batch

        def settle(i):
            mine = lax.dynamic_slice(x, (i, me * share, 0), (1, share, d))[0]
            h = (wide(mine) + wide(sums[i])).astype(jnp.bfloat16)
            hs[i] = h
            return normed(h, gain_m)

        for i in range(batch):
            term = attended(x, i, gain, turn, wq, wk, wv, wo)
            if i > 1:
                term, sums[i - 2] = tie((term, sums[i - 2]))
                b = settle(i - 2)
                b, term = tie((b, term))
                bs[i - 2] = gathered(b)
            term, gain = tie((term, gain))
            sums[i] = scattered(term)

        def late(i, after):
            after, sums[i] = tie((after, sums[i]))
            b, after = tie((settle(i), after))
            bs[i] = gathered(b)
            return after

        def finished(i, total, after):
            after, total = tie((after, total))
            part, after = tie(((wide(hs[i]) + wide(total)).astype(jnp.bfloat16), after))
            return gathered(part), after

        final, second, flying = [None] * batch, [None] * batch, None
        for i in range(batch):
            low, high = gated(bs[i], w_gate, w_up, 0, 1 if flying is None else 2), None
            if i == 1:
                low = late(3, low)
            if flying is not None:
                low, got = tie((low, flying.got))
                far, low = tie((flying.far(got), low))
                far = flying.send_far(far)
                low, b = tie((low, bs[i]))
                high = gated(b, w_gate, w_up, 1, 2)
                high, far = tie((high, far))
                near, high = tie((flying.near(got, far), high))
                near = flying.send_near(near)
            if i == 3:
                final[2], low = finished(2, second[2], low)
                break
            if i == 2:
                y, high = tie((placed(None, final[0], batch, 0, 0, d), high))
            term = downed(low, high, w_down)
            if flying is not None:
                term, near = tie((term, near))
                final[i - 1], bs[i + 1] = finished(i - 1, flying.total(got, near), bs[i + 1])
            flying = None
            if i < 2:
                flying = Sum(term)
            else:
                term, bs[i + 1] = tie((term, bs[i + 1]))
                second[i] = scattered(term)
            if i == 0:
                bs[1] = late(2, bs[1])

        middle = d // 2
        one = Sum(downed(low, None, w_down, 0, 2), low)
        two = downed(one.after, None, w_down, 1, 2)
        got, two = tie((one.got, two))
        two = Sum(two, got)
        got = two.after
        far = one.send_far(tie(one.far(got)))
        got_two = two.got
        far_two = two.send_far(tie(two.far(got_two)))
        far, y = tie((far, placed(y, final[1], batch, 1, 0, d)))
        near = one.send_near(tie(one.near(got, far)))
        far_two = tie(far_two)
        near_two = two.send_near(tie(two.near(got_two, far_two)))
        part = (wide(hs[-1][:, :middle]) + one.total(got, near)).astype(jnp.bfloat16)
        near_two, y = tie((near_two, placed(y, final[2], batch, 2, 0, d)))
        ends = [Spread(part)]
        ends.append(Spread((wide(hs[-1][:, middle:]) + two.total(got_two, near_two)).astype(jnp.bfloat16)))
        ends[0].forward()
        y, ends[1].near = tie((y, ends[1].near))
        ends[1].forward()
        for half, end in enumerate(ends):
            for at, rows_there in end.pieces():
                y = lax.dynamic_update_slice(y, rows_there[None], (batch - 1, at, half * middle))
        return y

    tokens, whole, columns, rows_of = P("dp", None, None), P(None), P(None, "tp"), P("tp", None)
    return jax.shard_map(
        step,
        mesh=mesh,
        in_specs=(tokens, whole, columns, columns, columns, rows_of, whole, columns, columns, rows_of),
        out_specs=tokens,
        check_vma=False,
    )
```
